32 devices in a mesh: slab: 8 (over z, y), plane: 4 (over x, core).
Axes of the slice: x: 2, y: 2, z: 4, core: 2. Of those that a mesh axis runs over, the one named last changes fastest.
Arguments:
- a_blocks: bfloat16 [4, 96, 7, 128, 128], P('plane', 'slab'), may hold values from -0.1875 to 0.1875
- a_cols: int32 [4, 96, 7], P('plane', 'slab'), may hold values from 0 to 95, as said below
- p_blocks: bfloat16 [4, 96, 4, 128, 128], P('plane', 'slab'), may hold values from -0.75 to 0.75
- p_cols: int32 [4, 96, 4], replicated, may hold values from 0 to 31, as said below
- coarse_slot: int32 [8, 4], replicated, may hold values from 0 to 3, each once within a row
Outputs:
- coarse_op: float32 [4, 8, 128, 2560], P('plane', 'slab')
The draws below stay inside these ranges and needn't reach their ends.
Inputs may be any that keep to these rules, and one draw needn't show every extreme that they name: `a_cols`: row g = s*12 + r of column p names 7 distinct block rows of column p, among them g itself; they lie in s*12 to s*12 + 11, or, if r < 4, in the 4 rows just below s*12, or, if r >= 8, in the 4 rows from (s+1)*12 on. `p_cols`: row g = s*12 + r names 4 distinct coarse blocks of s*4 to s*4 + 3, or, if r < 4, also of the 4 blocks before, or, if r >= 8, of the 4 blocks after. `coarse_slot`: each row is a permutation of 0 to 3.
All inputs are finite; a program needn't handle non-finite values.
Results may differ from the reference program's by a relative error of at most 0.0029.
Values may be sent and summed in bfloat16 or wider, within the bound.
A program may use at most 192 MiB of HBM per device.

```python
import jax
import jax.numpy as jnp
from jax import lax

B = 128
BR = 12
GHOST = 4
KA = 7
KP = 4
CB = 1
PLANES = 4
SLABS = 8
CS = 4
NBS = 96
WIN = 2560


def draw_a_cols(key, part):
    rows = jnp.arange(NBS, dtype=jnp.int32)
    slab = rows // BR
    inner = rows % BR
    cand = jnp.arange(BR + 2 * GHOST, dtype=jnp.int32)
    own = (cand[None, :] >= GHOST) & (cand[None, :] < GHOST + BR)
    lower = (cand[None, :] < GHOST) & (inner[:, None] < GHOST) & (slab[:, None] > 0)
    upper = (cand[None, :] >= GHOST + BR) & (inner[:, None] >= BR - GHOST) & (slab[:, None] < SLABS - 1)
    valid = own | lower | upper
    noise = jax.random.randint(key, (PLANES, NBS, BR + 2 * GHOST), 0, 2 ** 20, dtype=jnp.int32)
    score = noise * 128 + cand[None, None, :]
    score = score + jnp.where(lower | upper, 2 ** 27, 0)[None]
    score = score + jnp.where(cand[None, :] == GHOST + inner[:, None], 2 ** 29, 0)[None]
    score = jnp.where(valid[None], score, -1)
    picked = lax.top_k(score, KA)[1].astype(jnp.int32)
    return (slab[None, :, None] * BR - GHOST + picked).astype(jnp.int32)


def draw_p_cols(key, part):
    rows = jnp.arange(NBS, dtype=jnp.int32)
    slab = rows // BR
    inner = rows % BR
    cand = jnp.arange(3 * CS, dtype=jnp.int32)
    own = (cand[None, :] >= CS) & (cand[None, :] < 2 * CS)
    lower = (cand[None, :] < CS) & (inner[:, None] < GHOST) & (slab[:, None] > 0)
    upper = (cand[None, :] >= 2 * CS) & (inner[:, None] >= BR - GHOST) & (slab[:, None] < SLABS - 1)
    valid = own | lower | upper
    noise = jax.random.randint(key, (PLANES, NBS, 3 * CS), 0, 2 ** 20, dtype=jnp.int32)
    score = jnp.where(valid[None], noise * 64 + cand[None, None, :], -1)
    picked = lax.top_k(score, KP)[1].astype(jnp.int32)
    return ((slab[None, :, None] - 1) * CS + picked).astype(jnp.int32)


def shard_levels(key, extent, split, least, high):
    loudness, own = 1.0, jax.random.fold_in(key, 6)
    for dim, blocks in split:
        heights = jnp.exp(jax.random.uniform(jax.random.fold_in(own, dim), (blocks,), jnp.float32, least / len(split), high / len(split)))
        loudness = loudness * jnp.repeat(heights, extent[dim] // blocks).reshape([-1 if axis == dim else 1 for axis in range(len(extent))])
    return loudness


def bell_draw(own_key, dims, scale, bound, shards=(), held_as=jnp.bfloat16):
    array = scale * jax.random.normal(own_key, dims, jnp.float32)
    if shards:
        array = array * shard_levels(own_key, dims, shards, -0.22, 0.18)
    return jnp.clip(array, -bound, bound).astype(held_as)


def setup_inputs(seed: int = 0) -> dict:
    arg_keys = jax.random.split(jax.random.key(seed), 6)
    a_blocks = bell_draw(arg_keys[0], (PLANES, NBS, KA, B, B), (B * KA) ** -0.5, 0.1875, ((0, 4), (1, 8)))
    a_cols = draw_a_cols(jax.random.fold_in(arg_keys[5], 71), 0)
    p_blocks = bell_draw(arg_keys[2], (PLANES, NBS, KP, B, B), 0.125, 0.75, ((0, 4), (1, 8)))
    p_cols = draw_p_cols(jax.random.fold_in(arg_keys[5], 71), 0)
    coarse_slot = jax.vmap(lambda own: jax.random.permutation(own, CS))(jax.random.split(arg_keys[4], SLABS)).reshape((SLABS, CS)).astype(jnp.int32)
    return {"a_blocks": a_blocks, "a_cols": a_cols, "p_blocks": p_blocks, "p_cols": p_cols, "coarse_slot": coarse_slot}


def window_rows(blocks, cols, slot_table, slab):
    count = blocks.shape[0]
    owner = jnp.clip(cols // CS, 0, SLABS - 1)
    inside = cols % CS
    slot = slot_table[owner, inside]
    place = (cols // CS - slab + 1) * CS + slot
    onehot = (place[:, :, None] == jnp.arange(3 * CS, dtype=jnp.int32)[None, None, :]).astype(jnp.float32)
    dense = jnp.einsum('nkw,nkab->nawb', onehot, blocks.astype(jnp.float32))
    return dense.reshape(count, B, 3 * CS * B).astype(jnp.bfloat16)


def reference(a_blocks, a_cols, p_blocks, p_cols, coarse_slot):
    width = 3 * CS * B
    p_padded = jnp.pad(p_blocks, ((0, 0), (GHOST, GHOST), (0, 0), (0, 0), (0, 0)))
    c_padded = jnp.pad(p_cols, ((0, 0), (GHOST, GHOST), (0, 0)))

    def slab_part(slab):
        start = (slab * BR).astype(jnp.int32)
        near_blocks = lax.dynamic_slice_in_dim(p_padded, start, BR + 2 * GHOST, 1)
        near_cols = lax.dynamic_slice_in_dim(c_padded, start, BR + 2 * GHOST, 1)
        dense = window_rows(near_blocks.reshape(-1, KP, B, B), near_cols.reshape(-1, KP), coarse_slot, slab)
        dense = dense.reshape(PLANES, BR + 2 * GHOST, B, width)
        own_a = lax.dynamic_slice_in_dim(a_blocks, start, BR, 1)
        local = lax.dynamic_slice_in_dim(a_cols, start, BR, 1) - (start - GHOST)
        total = jnp.zeros((PLANES, BR, B, width), jnp.float32)
        for k in range(KA):
            picked = jax.vmap(lambda d, i: d[i])(dense, local[:, :, k])
            total = total + jnp.einsum('prab,prbw->praw', own_a[:, :, k].astype(jnp.float32), picked.astype(jnp.float32))
        product = total.astype(jnp.bfloat16)
        own_rows = dense[:, GHOST:GHOST + BR].reshape(-1, width)
        return lax.dot_general(own_rows, product.reshape(-1, width), (((0,), (0,)), ((), ())), preferred_element_type=jnp.float32)

    parts = lax.map(slab_part, jnp.arange(SLABS, dtype=jnp.int32))
    groups = parts.reshape(SLABS, 3, CS * B, width)
    middle = groups[:, 1]
    empty = jnp.zeros((1, CS * B, width), jnp.float32)
    below = jnp.concatenate([empty, groups[:-1, 2]], axis=0)
    above = jnp.concatenate([groups[1:, 0], empty], axis=0)
    edge = CS * B
    full = jnp.pad(middle, ((0, 0), (0, 0), (edge, edge)))
    full = full + jnp.pad(below, ((0, 0), (0, 0), (0, 2 * edge)))
    full = full + jnp.pad(above, ((0, 0), (0, 0), (2 * edge, 0)))
    full = full.reshape(SLABS, PLANES, CB, B, WIN)
    return jnp.transpose(full, (1, 0, 2, 3, 4)).reshape(PLANES, SLABS * CB, B, WIN)
```

```python
import functools

import jax
import jax.numpy as jnp
from jax import lax
from jax.experimental import pallas as pl
from jax.experimental.pallas import tpu as pltpu
from jax.sharding import PartitionSpec as P

GHOST = 4
MESH = pl.DeviceIdType.MESH


def kernel(dims, table, picks, a_hbm, p_hbm, out, *scratch):
    slabs, planes, rows, links, kp, block, coarse, owned = dims
    stages = planes.bit_length() - 1
    edge = coarse * block
    width = 3 * edge
    chunks = 3
    (a_own, p_own, p_low, p_high, pt, q, qt0, qt1, qt2, ap, final,
     send_c, recv_c, local_sem, halo_send, halo_recv, c_sem, c_got) = scratch[:18]
    rest = scratch[18:]
    send_b, recv_b, keep_b, b_sem, b_got = (rest[i * stages : (i + 1) * stages] for i in range(5))
    slab = lax.axis_index("slab")
    me = lax.axis_index("plane")
    bits = [(me // (1 << t)) % 2 for t in range(stages)]
    partners = [me + (1 - 2 * bits[t]) * (1 << t) for t in range(stages)]
    has_low = slab > 0
    has_high = slab < slabs - 1

    copy_a = pltpu.make_async_copy(a_hbm, a_own, local_sem.at[0])
    copy_p = pltpu.make_async_copy(p_hbm, p_own.at[pl.ds(0, rows * kp)], local_sem.at[1])
    copy_p.start()
    copy_a.start()

    barrier = pltpu.get_barrier_semaphore()
    for t in range(stages):
        pl.semaphore_signal(barrier, inc=1, device_id=(slab, partners[t]), device_id_type=MESH)

    @pl.when(has_low)
    def _():
        pl.semaphore_signal(barrier, inc=1, device_id=(slab - 1, me), device_id_type=MESH)

    @pl.when(has_high)
    def _():
        pl.semaphore_signal(barrier, inc=1, device_id=(slab + 1, me), device_id_type=MESH)

    neighbours = stages + jnp.where(has_low, 1, 0) + jnp.where(has_high, 1, 0)
    pl.semaphore_wait(barrier, neighbours)

    ghosts = GHOST * kp
    halo_up = pltpu.make_async_remote_copy(
        src_ref=p_hbm.at[pl.ds((rows - GHOST) * kp, ghosts)],
        dst_ref=p_low.at[pl.ds(0, ghosts)],
        send_sem=halo_send.at[0], recv_sem=halo_recv.at[0],
        device_id=(slab + 1, me), device_id_type=MESH)
    halo_down = pltpu.make_async_remote_copy(
        src_ref=p_hbm.at[pl.ds(0, ghosts)],
        dst_ref=p_high.at[pl.ds(0, ghosts)],
        send_sem=halo_send.at[1], recv_sem=halo_recv.at[1],
        device_id=(slab - 1, me), device_id_type=MESH)

    @pl.when(has_high)
    def _():
        halo_up.start()

    @pl.when(has_low)
    def _():
        halo_down.start()

    zero = jnp.zeros((block, block), jnp.bfloat16)
    p_own[rows * kp] = zero
    p_low[ghosts] = zero
    p_high[ghosts] = zero

    @pl.when(slab == 0)
    def _():
        p_low[...] = jnp.zeros_like(p_low)
        recv_c[1] = jnp.zeros(recv_c.shape[1:], recv_c.dtype)

    @pl.when(slab == slabs - 1)
    def _():
        p_high[...] = jnp.zeros_like(p_high)
        recv_c[0] = jnp.zeros(recv_c.shape[1:], recv_c.dtype)

    def spread(first, count, blocks):
        def body(i, _):
            n = first + i
            for w in range(3 * coarse):
                q[n, :, w * block : (w + 1) * block] = blocks[table[n, w]]
            return 0

        lax.fori_loop(0, count, body, 0)

    def multiply(first, count):
        def body(i, _):
            g = first + i
            left = jnp.concatenate([a_own[g * links + k] for k in range(links)], axis=1)
            at = [picks[g, k] for k in range(links)]
            for c in range(chunks):
                right = jnp.concatenate(
                    [q[at[k], :, c * edge : (c + 1) * edge] for k in range(links)], axis=0)
                ap[pl.ds(pl.multiple_of(g * block, block), block), c * edge : (c + 1) * edge] = jnp.dot(
                    left, right, preferred_element_type=jnp.float32).astype(jnp.bfloat16)
            return 0

        lax.fori_loop(0, count, body, 0)

    copy_p.wait()
    spread(GHOST, rows, p_own)

    def flip(b, _):
        pt[b] = p_own[b].T
        return 0

    lax.fori_loop(0, rows * kp + 1, flip, 0)
    parts = ((qt0, 0, GHOST), (qt1, 0, rows), (qt2, rows - GHOST, GHOST))
    for j, (qt, first, count) in enumerate(parts):
        for i in range(count):
            for slot in range(coarse):
                qt[slot // owned, (slot % owned) * block : (slot % owned + 1) * block, i * block : (i + 1) * block] = (
                    pt[table[GHOST + first + i, j * coarse + slot]])
    copy_a.wait()
    multiply(GHOST, rows - 2 * GHOST)

    def stage_copy(t, j, c):
        return pltpu.make_async_remote_copy(
            src_ref=send_b[t].at[j, c], dst_ref=recv_b[t].at[j, c],
            send_sem=b_sem[t].at[j, c], recv_sem=b_got[t].at[j, c],
            device_id=(slab, partners[t]), device_id_type=MESH)

    def final_copy(j, c):
        return pltpu.make_async_remote_copy(
            src_ref=send_c.at[j, c], dst_ref=recv_c.at[j, c],
            send_sem=c_sem.at[j, c], recv_sem=c_got.at[j, c],
            device_id=(slab - 1 if j == 0 else slab + 1, me), device_id_type=MESH)

    def form(j):
        qt, first, count = parts[j]
        half = planes // 2
        for c in range(chunks):
            right = ap[first * block : (first + count) * block, c * edge : (c + 1) * edge]
            for i in range(half):
                send_b[0][j, c, i] = jnp.dot(
                    qt[1 - bits[0] + 2 * i], right, preferred_element_type=jnp.float32).astype(jnp.bfloat16)
            stage_copy(0, j, c).start()
            for i in range(half):
                keep_b[0][j, c, i] = jnp.dot(
                    qt[bits[0] + 2 * i], right, preferred_element_type=jnp.float32)

    def fold(t, j):
        for c in range(chunks):
            stage_copy(t - 1, j, c).wait_recv()
            for i in range(planes >> (t + 1)):
                at = 1 - bits[t] + 2 * i
                send_b[t][j, c, i] = (
                    keep_b[t - 1][j, c, at] + recv_b[t - 1][j, c, at].astype(jnp.float32)).astype(jnp.bfloat16)
            stage_copy(t, j, c).start()
            for i in range(planes >> (t + 1)):
                at = bits[t] + 2 * i
                keep_b[t][j, c, i] = keep_b[t - 1][j, c, at] + recv_b[t - 1][j, c, at].astype(jnp.float32)

    def finish(j):
        for c in range(chunks):
            stage_copy(stages - 1, j, c).wait_recv()
            value = keep_b[stages - 1][j, c, 0] + recv_b[stages - 1][j, c, 0].astype(jnp.float32)
            if j == 1:
                final[c] = value
            else:
                send_c[j // 2, c] = value.astype(jnp.bfloat16)

                @pl.when(has_low if j == 0 else has_high)
                def _():
                    final_copy(j // 2, c).start()

    @pl.when(has_low)
    def _():
        halo_up.wait_recv()

    spread(0, GHOST, p_low)
    multiply(0, GHOST)
    form(0)
    for t in range(1, stages):
        fold(t, 0)

    @pl.when(has_high)
    def _():
        halo_down.wait_recv()

    spread(GHOST + rows, GHOST, p_high)
    multiply(rows - GHOST, GHOST)
    form(2)
    finish(0)
    for t in range(1, stages):
        fold(t, 2)
    form(1)
    finish(2)
    for t in range(1, stages):
        fold(t, 1)
    finish(1)

    @pl.when(has_high)
    def _():
        for c in range(chunks):
            final_copy(0, c).wait_recv()

    @pl.when(has_low)
    def _():
        for c in range(chunks):
            final_copy(1, c).wait_recv()

    for o in range(5):
        terms = []
        if 0 <= o - 1 < chunks:
            terms.append(final[o - 1])
        if o < chunks:
            terms.append(recv_c[1, o].astype(jnp.float32))
        if o >= 2:
            terms.append(recv_c[0, o - 2].astype(jnp.float32))
        out[:, o * edge : (o + 1) * edge] = functools.reduce(jnp.add, terms)

    @pl.when(has_high)
    def _():
        halo_up.wait_send()
        for c in range(chunks):
            final_copy(1, c).wait_send()

    @pl.when(has_low)
    def _():
        halo_down.wait_send()
        for c in range(chunks):
            final_copy(0, c).wait_send()

    for t in range(stages):
        for j in range(3):
            for c in range(chunks):
                stage_copy(t, j, c).wait_send()


def tables(a_cols, p_cols, coarse_slot, rows, coarse):
    slab = lax.axis_index("slab")
    column = lax.axis_index("plane")
    start = slab * rows
    kp = p_cols.shape[2]
    mine = lax.dynamic_slice_in_dim(p_cols, column, 1, 0)[0]
    mine = jnp.pad(mine, ((GHOST, GHOST), (0, 0)))
    cols = lax.dynamic_slice_in_dim(mine, start, rows + 2 * GHOST, 0)
    slots = jnp.pad(coarse_slot, ((1, 1), (0, 0)))
    nearby = lax.dynamic_slice_in_dim(slots, slab, 3, 0).reshape(-1)
    relative = cols - (slab - 1) * coarse
    lanes = jnp.arange(3 * coarse, dtype=jnp.int32)
    slot = jnp.sum(jnp.where(relative[:, :, None] == lanes, nearby, 0), axis=-1)
    place = relative // coarse * coarse + slot
    match = place[:, :, None] == lanes
    which = jnp.max(jnp.where(match, jnp.arange(kp, dtype=jnp.int32)[None, :, None], -1), axis=1)
    n = jnp.arange(rows + 2 * GHOST, dtype=jnp.int32)
    low, high = n < GHOST, n >= GHOST + rows
    base = jnp.where(low, n, jnp.where(high, n - GHOST - rows, n - GHOST)) * kp
    none = jnp.where(low | high, GHOST * kp, rows * kp)
    table = jnp.where(which >= 0, base[:, None] + which, none[:, None])
    return table, a_cols[0] - (start - GHOST)


def on_device(a_blocks, a_cols, p_blocks, p_cols, coarse_slot):
    rows, links, block = a_blocks.shape[1:4]
    kp = p_blocks.shape[2]
    coarse = coarse_slot.shape[1]
    slabs = lax.axis_size("slab")
    planes = lax.axis_size("plane")
    owned = coarse // planes
    stages = planes.bit_length() - 1
    assert planes == 1 << stages and stages > 0
    edge = coarse * block
    width = 3 * edge
    high = owned * block
    table, picks = tables(a_cols, p_cols, coarse_slot, rows, coarse)
    dims = (slabs, planes, rows, links, kp, block, coarse, owned)
    bf, f32 = jnp.bfloat16, jnp.float32
    vmem = pltpu.VMEM
    dma = pltpu.SemaphoreType.DMA
    shape = lambda t: (3, 3, planes >> (t + 1), high, edge)
    scratch = [
        vmem((rows * links, block, block), bf),
        vmem((rows * kp + 1, block, block), bf),
        vmem((GHOST * kp + 1, block, block), bf),
        vmem((GHOST * kp + 1, block, block), bf),
        vmem((rows * kp + 1, block, block), bf),
        vmem((rows + 2 * GHOST, block, width), bf),
        vmem((planes, high, GHOST * block), bf),
        vmem((planes, high, rows * block), bf),
        vmem((planes, high, GHOST * block), bf),
        vmem((rows * block, width), bf),
        vmem((3, high, edge), f32),
        vmem((2, 3, high, edge), bf),
        vmem((2, 3, high, edge), bf),
        dma((2,)), dma((2,)), dma((2,)), dma((2, 3)), dma((2, 3)),
    ]
    scratch += [vmem(shape(t), bf) for t in range(stages)]
    scratch += [vmem(shape(t), bf) for t in range(stages)]
    scratch += [vmem(shape(t), f32) for t in range(stages)]
    scratch += [dma((3, 3)) for t in range(2 * stages)]
    smem = pl.BlockSpec(memory_space=pltpu.SMEM)
    anywhere = pl.BlockSpec(memory_space=pl.ANY)
    result = pl.pallas_call(
        functools.partial(kernel, dims),
        out_shape=jax.ShapeDtypeStruct((high, 5 * edge), f32),
        in_specs=[smem, smem, anywhere, anywhere],
        out_specs=pl.BlockSpec(memory_space=pltpu.VMEM),
        scratch_shapes=scratch,
        compiler_params=pltpu.CompilerParams(
            collective_id=0, has_side_effects=True, vmem_limit_bytes=62 * 1024 * 1024),
    )(table, picks, a_blocks.reshape(rows * links, block, block), p_blocks.reshape(rows * kp, block, block))
    return result.reshape(1, owned, block, 5 * edge)


def solution(mesh):
    return jax.shard_map(
        on_device,
        mesh=mesh,
        in_specs=(
            P("plane", "slab", None, None, None),
            P("plane", "slab", None),
            P("plane", "slab", None, None, None),
            P(),
            P(),
        ),
        out_specs=P("plane", "slab", None, None),
        check_vma=False,
    )
```

```python
import functools

import jax
import jax.numpy as jnp
from jax import lax
from jax.experimental import pallas as pl
from jax.experimental.pallas import tpu as pltpu
from jax.sharding import PartitionSpec as P

GHOST = 4
MESH = pl.DeviceIdType.MESH


def kernel(dims, a_cols, p_cols, slots, a_hbm, p_hbm, out, *scratch):
    slabs, planes, rows, links, kp, block, coarse, owned = dims
    stages = planes.bit_length() - 1
    edge = coarse * block
    width = 3 * edge
    chunks = 3
    (a_own, p_own, p_low, p_high, pt, q, qt0, qt1, qt2, ap, final,
     send_c, recv_c, local_sem, halo_send, halo_recv, c_sem, c_got, table) = scratch[:19]
    rest = scratch[19:]
    send_b, recv_b, keep_b, b_sem, b_got = (rest[i * stages : (i + 1) * stages] for i in range(5))
    slab = lax.axis_index("slab")
    me = lax.axis_index("plane")
    bits = [(me // (1 << t)) % 2 for t in range(stages)]
    partners = [me + (1 - 2 * bits[t]) * (1 << t) for t in range(stages)]
    has_low = slab > 0
    has_high = slab < slabs - 1

    copy_a = pltpu.make_async_copy(a_hbm, a_own, local_sem.at[0])
    copy_p = pltpu.make_async_copy(p_hbm, p_own.at[pl.ds(0, rows * kp)], local_sem.at[1])
    copy_p.start()
    copy_a.start()

    barrier = pltpu.get_barrier_semaphore()
    for t in range(stages):
        pl.semaphore_signal(barrier, inc=1, device_id=(slab, partners[t]), device_id_type=MESH)

    @pl.when(has_low)
    def _():
        pl.semaphore_signal(barrier, inc=1, device_id=(slab - 1, me), device_id_type=MESH)

    @pl.when(has_high)
    def _():
        pl.semaphore_signal(barrier, inc=1, device_id=(slab + 1, me), device_id_type=MESH)

    neighbours = stages + jnp.where(has_low, 1, 0) + jnp.where(has_high, 1, 0)
    pl.semaphore_wait(barrier, neighbours)

    ghosts = GHOST * kp
    halo_up = pltpu.make_async_remote_copy(
        src_ref=p_hbm.at[pl.ds((rows - GHOST) * kp, ghosts)],
        dst_ref=p_low.at[pl.ds(0, ghosts)],
        send_sem=halo_send.at[0], recv_sem=halo_recv.at[0],
        device_id=(slab + 1, me), device_id_type=MESH)
    halo_down = pltpu.make_async_remote_copy(
        src_ref=p_hbm.at[pl.ds(0, ghosts)],
        dst_ref=p_high.at[pl.ds(0, ghosts)],
        send_sem=halo_send.at[1], recv_sem=halo_recv.at[1],
        device_id=(slab - 1, me), device_id_type=MESH)

    @pl.when(has_high)
    def _():
        halo_up.start()

    start = slab * rows
    total = p_cols.shape[2]

    def chart(n, _):
        row = jnp.clip(start - GHOST + n, 0, total - 1)
        place = []
        for m in range(kp):
            col = p_cols[me, m, row]
            near = col // coarse
            place.append((near - slab + 1) * coarse + slots[col % coarse, near])
        low, high = n < GHOST, n >= GHOST + rows
        base = jnp.where(low, n, jnp.where(high, n - GHOST - rows, n - GHOST)) * kp
        none = jnp.where(low | high, GHOST * kp, rows * kp)
        for w in range(3 * coarse):
            value = none
            for m in range(kp):
                value = jnp.where(place[m] == w, base + m, value)
            table[n, w] = value
        return 0

    lax.fori_loop(0, rows + 2 * GHOST, chart, 0)

    zero = jnp.zeros((block, block), jnp.bfloat16)
    p_own[rows * kp] = zero
    p_low[ghosts] = zero
    p_high[ghosts] = zero

    @pl.when(slab == 0)
    def _():
        p_low[...] = jnp.zeros_like(p_low)
        recv_c[1] = jnp.zeros(recv_c.shape[1:], recv_c.dtype)

    @pl.when(slab == slabs - 1)
    def _():
        p_high[...] = jnp.zeros_like(p_high)
        recv_c[0] = jnp.zeros(recv_c.shape[1:], recv_c.dtype)

    def spread(first, count, blocks):
        def body(i, _):
            n = first + i
            for w in range(3 * coarse):
                q[n, :, w * block : (w + 1) * block] = blocks[table[n, w]]
            return 0

        lax.fori_loop(0, count, body, 0)

    def multiply(first, count):
        def body(i, _):
            g = first + i
            left = jnp.concatenate([a_own[g * links + k] for k in range(links)], axis=1)
            at = [jnp.clip(a_cols[k, 0, g] - (start - GHOST), 0, rows + 2 * GHOST - 1) for k in range(links)]
            for c in range(chunks):
                right = jnp.concatenate(
                    [q[at[k], :, c * edge : (c + 1) * edge] for k in range(links)], axis=0)
                ap[pl.ds(pl.multiple_of(g * block, block), block), c * edge : (c + 1) * edge] = jnp.dot(
                    left, right, preferred_element_type=jnp.float32).astype(jnp.bfloat16)
            return 0

        lax.fori_loop(0, count, body, 0)

    copy_p.wait()
    spread(GHOST, rows, p_own)

    def flip(b, _):
        pt[b] = p_own[b].T
        return 0

    lax.fori_loop(0, rows * kp + 1, flip, 0)
    parts = ((qt0, 0, GHOST), (qt1, 0, rows), (qt2, rows - GHOST, GHOST))
    for j, (qt, first, count) in enumerate(parts):
        for i in range(count):
            for slot in range(coarse):
                qt[slot // owned, (slot % owned) * block : (slot % owned + 1) * block, i * block : (i + 1) * block] = (
                    pt[table[GHOST + first + i, j * coarse + slot]])
    copy_a.wait()
    multiply(GHOST, rows - 2 * GHOST)

    def stage_copy(t, j, c):
        return pltpu.make_async_remote_copy(
            src_ref=send_b[t].at[j, c], dst_ref=recv_b[t].at[j, c],
            send_sem=b_sem[t].at[j, c], recv_sem=b_got[t].at[j, c],
            device_id=(slab, partners[t]), device_id_type=MESH)

    def final_copy(j, c):
        return pltpu.make_async_remote_copy(
            src_ref=send_c.at[j, c], dst_ref=recv_c.at[j, c],
            send_sem=c_sem.at[j, c], recv_sem=c_got.at[j, c],
            device_id=(slab - 1 if j == 0 else slab + 1, me), device_id_type=MESH)

    def form(j):
        qt, first, count = parts[j]
        half = planes // 2
        for c in range(chunks):
            right = ap[first * block : (first + count) * block, c * edge : (c + 1) * edge]
            for i in range(half):
                send_b[0][j, c, i] = jnp.dot(
                    qt[1 - bits[0] + 2 * i], right, preferred_element_type=jnp.float32).astype(jnp.bfloat16)
            stage_copy(0, j, c).start()
            for i in range(half):
                keep_b[0][j, c, i] = jnp.dot(
                    qt[bits[0] + 2 * i], right, preferred_element_type=jnp.float32)

    def fold(t, j):
        for c in range(chunks):
            stage_copy(t - 1, j, c).wait_recv()
            for i in range(planes >> (t + 1)):
                at = 1 - bits[t] + 2 * i
                send_b[t][j, c, i] = (
                    keep_b[t - 1][j, c, at] + recv_b[t - 1][j, c, at].astype(jnp.float32)).astype(jnp.bfloat16)
            stage_copy(t, j, c).start()
            for i in range(planes >> (t + 1)):
                at = bits[t] + 2 * i
                keep_b[t][j, c, i] = keep_b[t - 1][j, c, at] + recv_b[t - 1][j, c, at].astype(jnp.float32)

    def finish(j, which):
        for c in which:
            stage_copy(stages - 1, j, c).wait_recv()
            value = keep_b[stages - 1][j, c, 0] + recv_b[stages - 1][j, c, 0].astype(jnp.float32)
            if j == 1:
                final[c] = value
            else:
                send_c[j // 2, c] = value.astype(jnp.bfloat16)

                @pl.when(has_low if j == 0 else has_high)
                def _():
                    final_copy(j // 2, c).start()

    @pl.when(has_high)
    def _():
        halo_up.wait_send()

    @pl.when(has_low)
    def _():
        halo_down.start()
        halo_up.wait_recv()

    spread(0, GHOST, p_low)
    multiply(0, GHOST)
    form(0)
    for t in range(1, stages):
        fold(t, 0)
    finish(0, range(chunks - 1))

    @pl.when(has_high)
    def _():
        halo_down.wait_recv()

    spread(GHOST + rows, GHOST, p_high)
    multiply(rows - GHOST, GHOST)
    finish(0, range(chunks - 1, chunks))
    form(2)
    for t in range(1, stages):
        fold(t, 2)
    form(1)
    for t in range(1, stages):
        fold(t, 1)
    finish(2, range(chunks))
    finish(1, range(chunks))

    @pl.when(has_high)
    def _():
        for c in range(chunks):
            final_copy(0, c).wait_recv()

    @pl.when(has_low)
    def _():
        for c in range(chunks):
            final_copy(1, c).wait_recv()

    for o in range(5):
        terms = []
        if 0 <= o - 1 < chunks:
            terms.append(final[o - 1])
        if o < chunks:
            terms.append(recv_c[1, o].astype(jnp.float32))
        if o >= 2:
            terms.append(recv_c[0, o - 2].astype(jnp.float32))
        out[:, o * edge : (o + 1) * edge] = functools.reduce(jnp.add, terms)

    @pl.when(has_high)
    def _():
        for c in range(chunks):
            final_copy(1, c).wait_send()

    @pl.when(has_low)
    def _():
        halo_down.wait_send()
        for c in range(chunks):
            final_copy(0, c).wait_send()

    for t in range(stages):
        for j in range(3):
            for c in range(chunks):
                stage_copy(t, j, c).wait_send()


def on_device(a_blocks, a_cols, p_blocks, p_cols, coarse_slot):
    rows, links, block = a_blocks.shape[1:4]
    kp = p_blocks.shape[2]
    coarse = coarse_slot.shape[1]
    slabs = lax.axis_size("slab")
    planes = lax.axis_size("plane")
    owned = coarse // planes
    stages = planes.bit_length() - 1
    assert planes == 1 << stages and stages > 0
    edge = coarse * block
    width = 3 * edge
    high = owned * block
    dims = (slabs, planes, rows, links, kp, block, coarse, owned)
    bf, f32 = jnp.bfloat16, jnp.float32
    vmem = pltpu.VMEM
    dma = pltpu.SemaphoreType.DMA
    shape = lambda t: (3, 3, planes >> (t + 1), high, edge)
    scratch = [
        vmem((rows * links, block, block), bf),
        vmem((rows * kp + 1, block, block), bf),
        vmem((GHOST * kp + 1, block, block), bf),
        vmem((GHOST * kp + 1, block, block), bf),
        vmem((rows * kp + 1, block, block), bf),
        vmem((rows + 2 * GHOST, block, width), bf),
        vmem((planes, high, GHOST * block), bf),
        vmem((planes, high, rows * block), bf),
        vmem((planes, high, GHOST * block), bf),
        vmem((rows * block, width), bf),
        vmem((3, high, edge), f32),
        vmem((2, 3, high, edge), bf),
        vmem((2, 3, high, edge), bf),
        dma((2,)), dma((2,)), dma((2,)), dma((2, 3)), dma((2, 3)),
        pltpu.SMEM((rows + 2 * GHOST, 3 * coarse), jnp.int32),
    ]
    scratch += [vmem(shape(t), bf) for t in range(stages)]
    scratch += [vmem(shape(t), bf) for t in range(stages)]
    scratch += [vmem(shape(t), f32) for t in range(stages)]
    scratch += [dma((3, 3)) for t in range(2 * stages)]
    smem = pl.BlockSpec(memory_space=pltpu.SMEM)
    anywhere = pl.BlockSpec(memory_space=pl.ANY)
    result = pl.pallas_call(
        functools.partial(kernel, dims),
        out_shape=jax.ShapeDtypeStruct((high, 5 * edge), f32),
        in_specs=[smem, smem, smem, anywhere, anywhere],
        out_specs=pl.BlockSpec(memory_space=pltpu.VMEM),
        scratch_shapes=scratch,
        compiler_params=pltpu.CompilerParams(
            collective_id=0, has_side_effects=True, vmem_limit_bytes=62 * 1024 * 1024),
    )(a_cols.transpose(2, 0, 1), p_cols.transpose(0, 2, 1), coarse_slot.T, a_blocks.reshape(rows * links, block, block), p_blocks.reshape(rows * kp, block, block))
    return result.reshape(1, owned, block, 5 * edge)


def solution(mesh):
    return jax.shard_map(
        on_device,
        mesh=mesh,
        in_specs=(
            P("plane", "slab", None, None, None),
            P("plane", "slab", None),
            P("plane", "slab", None, None, None),
            P(),
            P(),
        ),
        out_specs=P("plane", "slab", None, None),
        check_vma=False,
    )
```

```python
import functools

import jax
import jax.numpy as jnp
from jax import lax
from jax.experimental import pallas as pl
from jax.experimental.pallas import tpu as pltpu
from jax.sharding import PartitionSpec as P

GHOST = 4
MESH = pl.DeviceIdType.MESH


def kernel(dims, a_cols_hbm, p_cols_hbm, slots_hbm, a_hbm, p_hbm, out, *scratch):
    slabs, planes, rows, links, kp, block, coarse, owned = dims
    stages = planes.bit_length() - 1
    edge = coarse * block
    width = 3 * edge
    chunks = 3
    (a_own, p_own, p_low, p_high, pt, q, qt0, qt1, qt2, ap, final,
     send_c, recv_c, local_sem, halo_send, halo_recv, c_sem, c_got, table, whole, out_sem, a_cols, p_cols, slots, index_sem) = scratch[:25]
    rest = scratch[25:]
    send_b, recv_b, keep_b, b_sem, b_got = (rest[i * stages : (i + 1) * stages] for i in range(5))
    slab = lax.axis_index("slab")
    me = lax.axis_index("plane")
    bits = [(me // (1 << t)) % 2 for t in range(stages)]
    partners = [me + (1 - 2 * bits[t]) * (1 << t) for t in range(stages)]
    has_low = slab > 0
    has_high = slab < slabs - 1

    copy_a = pltpu.make_async_copy(a_hbm, a_own, local_sem.at[0])
    copy_p = pltpu.make_async_copy(p_hbm, p_own.at[pl.ds(0, rows * kp)], local_sem.at[1])
    copy_index = [
        pltpu.make_async_copy(source, target, index_sem.at[i])
        for i, (source, target) in enumerate(
            ((a_cols_hbm, a_cols), (p_cols_hbm, p_cols), (slots_hbm, slots)))
    ]
    for copy in copy_index:
        copy.start()
    copy_p.start()
    copy_a.start()

    barrier = pltpu.get_barrier_semaphore()
    for t in range(stages):
        pl.semaphore_signal(barrier, inc=1, device_id=(slab, partners[t]), device_id_type=MESH)

    @pl.when(has_low)
    def _():
        pl.semaphore_signal(barrier, inc=1, device_id=(slab - 1, me), device_id_type=MESH)

    @pl.when(has_high)
    def _():
        pl.semaphore_signal(barrier, inc=1, device_id=(slab + 1, me), device_id_type=MESH)

    neighbours = stages + jnp.where(has_low, 1, 0) + jnp.where(has_high, 1, 0)
    pl.semaphore_wait(barrier, neighbours)

    ghosts = GHOST * kp
    halo_up = pltpu.make_async_remote_copy(
        src_ref=p_hbm.at[pl.ds((rows - GHOST) * kp, ghosts)],
        dst_ref=p_low.at[pl.ds(0, ghosts)],
        send_sem=halo_send.at[0], recv_sem=halo_recv.at[0],
        device_id=(slab + 1, me), device_id_type=MESH)
    halo_down = pltpu.make_async_remote_copy(
        src_ref=p_hbm.at[pl.ds(0, ghosts)],
        dst_ref=p_high.at[pl.ds(0, ghosts)],
        send_sem=halo_send.at[1], recv_sem=halo_recv.at[1],
        device_id=(slab - 1, me), device_id_type=MESH)

    @pl.when(has_high)
    def _():
        halo_up.start()

    start = slab * rows
    total = p_cols.shape[2]

    def chart(n, _):
        row = jnp.clip(start - GHOST + n, 0, total - 1)
        place = []
        for m in range(kp):
            col = p_cols[me, m, row]
            near = col // coarse
            place.append((near - slab + 1) * coarse + slots[col % coarse, near])
        low, high = n < GHOST, n >= GHOST + rows
        base = jnp.where(low, n, jnp.where(high, n - GHOST - rows, n - GHOST)) * kp
        none = jnp.where(low | high, GHOST * kp, rows * kp)
        for w in range(3 * coarse):
            value = none
            for m in range(kp):
                value = jnp.where(place[m] == w, base + m, value)
            table[n, w] = value
        return 0

    for copy in copy_index:
        copy.wait()
    lax.fori_loop(0, rows + 2 * GHOST, chart, 0)

    zero = jnp.zeros((block, block), jnp.bfloat16)
    p_own[rows * kp] = zero
    p_low[ghosts] = zero
    p_high[ghosts] = zero

    @pl.when(slab == 0)
    def _():
        p_low[...] = jnp.zeros_like(p_low)
        recv_c[1] = jnp.zeros(recv_c.shape[1:], recv_c.dtype)

    @pl.when(slab == slabs - 1)
    def _():
        p_high[...] = jnp.zeros_like(p_high)
        recv_c[0] = jnp.zeros(recv_c.shape[1:], recv_c.dtype)

    def spread(first, count, blocks):
        def body(i, _):
            n = first + i
            for w in range(3 * coarse):
                q[n, :, w * block : (w + 1) * block] = blocks[table[n, w]]
            return 0

        lax.fori_loop(0, count, body, 0)

    def multiply(first, count, columns):
        def body(i, _):
            g = first + i
            left = jnp.concatenate([a_own[g * links + k] for k in range(links)], axis=1)
            at = [jnp.clip(a_cols[k, 0, g] - (start - GHOST), 0, rows + 2 * GHOST - 1) for k in range(links)]
            for c in columns:
                right = jnp.concatenate(
                    [q[at[k], :, c * edge : (c + 1) * edge] for k in range(links)], axis=0)
                ap[pl.ds(pl.multiple_of(g * block, block), block), c * edge : (c + 1) * edge] = jnp.dot(
                    left, right, preferred_element_type=jnp.float32).astype(jnp.bfloat16)
            return 0

        lax.fori_loop(0, count, body, 0)

    copy_p.wait()
    spread(GHOST, rows, p_own)

    def flip(b, _):
        pt[b] = p_own[b].T
        return 0

    lax.fori_loop(0, rows * kp + 1, flip, 0)
    parts = ((qt0, 0, GHOST), (qt1, 0, rows), (qt2, rows - GHOST, GHOST))
    for j, (qt, first, count) in enumerate(parts):
        for i in range(count):
            for slot in range(coarse):
                qt[slot // owned, (slot % owned) * block : (slot % owned + 1) * block, i * block : (i + 1) * block] = (
                    pt[table[GHOST + first + i, j * coarse + slot]])
    copy_a.wait()
    multiply(GHOST, rows - 2 * GHOST, range(chunks))

    def stage_copy(t, j, c):
        return pltpu.make_async_remote_copy(
            src_ref=send_b[t].at[j, c], dst_ref=recv_b[t].at[j, c],
            send_sem=b_sem[t].at[j, c], recv_sem=b_got[t].at[j, c],
            device_id=(slab, partners[t]), device_id_type=MESH)

    def final_copy(j, c):
        return pltpu.make_async_remote_copy(
            src_ref=send_c.at[j, c], dst_ref=recv_c.at[j, c],
            send_sem=c_sem.at[j, c], recv_sem=c_got.at[j, c],
            device_id=(slab - 1 if j == 0 else slab + 1, me), device_id_type=MESH)

    def form(j, columns):
        qt, first, count = parts[j]
        half = planes // 2
        for c in columns:
            right = ap[first * block : (first + count) * block, c * edge : (c + 1) * edge]
            for i in range(half):
                send_b[0][j, c, i] = jnp.dot(
                    qt[1 - bits[0] + 2 * i], right, preferred_element_type=jnp.float32).astype(jnp.bfloat16)
            stage_copy(0, j, c).start()
            for i in range(half):
                keep_b[0][j, c, i] = jnp.dot(
                    qt[bits[0] + 2 * i], right, preferred_element_type=jnp.float32)

    def fold(t, j):
        for c in range(chunks):
            stage_copy(t - 1, j, c).wait_recv()
            for i in range(planes >> (t + 1)):
                at = 1 - bits[t] + 2 * i
                send_b[t][j, c, i] = (
                    keep_b[t - 1][j, c, at] + recv_b[t - 1][j, c, at].astype(jnp.float32)).astype(jnp.bfloat16)
            stage_copy(t, j, c).start()
            for i in range(planes >> (t + 1)):
                at = bits[t] + 2 * i
                keep_b[t][j, c, i] = keep_b[t - 1][j, c, at] + recv_b[t - 1][j, c, at].astype(jnp.float32)

    def finish(j, which):
        for c in which:
            stage_copy(stages - 1, j, c).wait_recv()
            value = keep_b[stages - 1][j, c, 0] + recv_b[stages - 1][j, c, 0].astype(jnp.float32)
            if j == 1:
                final[c] = value
            else:
                send_c[j // 2, c] = value.astype(jnp.bfloat16)

                @pl.when(has_low if j == 0 else has_high)
                def _():
                    final_copy(j // 2, c).start()

    @pl.when(has_high)
    def _():
        halo_up.wait_send()

    @pl.when(has_low)
    def _():
        halo_down.start()
        halo_up.wait_recv()

    spread(0, GHOST, p_low)
    for c in range(chunks):
        multiply(0, GHOST, (c,))
        form(0, (c,))
    for t in range(1, stages):
        fold(t, 0)
    finish(0, range(chunks - 1))

    @pl.when(has_high)
    def _():
        halo_down.wait_recv()

    spread(GHOST + rows, GHOST, p_high)
    for c in range(chunks):
        multiply(rows - GHOST, GHOST, (c,))
        form(2, (c,))
        if c == 0:
            finish(0, range(chunks - 1, chunks))
    for t in range(1, stages):
        fold(t, 2)
    form(1, range(chunks))
    for t in range(1, stages):
        fold(t, 1)
    finish(2, range(chunks))
    finish(1, range(chunks))

    @pl.when(has_high)
    def _():
        for c in range(chunks):
            final_copy(0, c).wait_recv()

    @pl.when(has_low)
    def _():
        for c in range(chunks):
            final_copy(1, c).wait_recv()

    def out_copy(o):
        return pltpu.make_async_copy(whole.at[o], out.at[:, pl.ds(o * edge, edge)], out_sem.at[o])

    for o in range(5):
        terms = []
        if 0 <= o - 1 < chunks:
            terms.append(final[o - 1])
        if o < chunks:
            terms.append(recv_c[1, o].astype(jnp.float32))
        if o >= 2:
            terms.append(recv_c[0, o - 2].astype(jnp.float32))
        whole[o] = functools.reduce(jnp.add, terms)
        out_copy(o).start()

    @pl.when(has_high)
    def _():
        for c in range(chunks):
            final_copy(1, c).wait_send()

    @pl.when(has_low)
    def _():
        halo_down.wait_send()
        for c in range(chunks):
            final_copy(0, c).wait_send()

    for t in range(stages):
        for j in range(3):
            for c in range(chunks):
                stage_copy(t, j, c).wait_send()
    for o in range(5):
        out_copy(o).wait()


def on_device(a_blocks, a_cols, p_blocks, p_cols, coarse_slot):
    rows, links, block = a_blocks.shape[1:4]
    kp = p_blocks.shape[2]
    coarse = coarse_slot.shape[1]
    slabs = lax.axis_size("slab")
    planes = lax.axis_size("plane")
    owned = coarse // planes
    stages = planes.bit_length() - 1
    assert planes == 1 << stages and stages > 0
    edge = coarse * block
    width = 3 * edge
    high = owned * block
    dims = (slabs, planes, rows, links, kp, block, coarse, owned)
    bf, f32 = jnp.bfloat16, jnp.float32
    vmem = pltpu.VMEM
    dma = pltpu.SemaphoreType.DMA
    shape = lambda t: (3, 3, planes >> (t + 1), high, edge)
    scratch = [
        vmem((rows * links, block, block), bf),
        vmem((rows * kp + 1, block, block), bf),
        vmem((GHOST * kp + 1, block, block), bf),
        vmem((GHOST * kp + 1, block, block), bf),
        vmem((rows * kp + 1, block, block), bf),
        vmem((rows + 2 * GHOST, block, width), bf),
        vmem((planes, high, GHOST * block), bf),
        vmem((planes, high, rows * block), bf),
        vmem((planes, high, GHOST * block), bf),
        vmem((rows * block, width), bf),
        vmem((3, high, edge), f32),
        vmem((2, 3, high, edge), bf),
        vmem((2, 3, high, edge), bf),
        dma((2,)), dma((2,)), dma((2,)), dma((2, 3)), dma((2, 3)),
        pltpu.SMEM((rows + 2 * GHOST, 3 * coarse), jnp.int32),
        vmem((5, high, edge), f32),
        dma((5,)),
        pltpu.SMEM((links, 1, rows), jnp.int32),
        pltpu.SMEM((planes, kp, p_cols.shape[1]), jnp.int32),
        pltpu.SMEM((coarse, slabs), jnp.int32),
        dma((3,)),
    ]
    scratch += [vmem(shape(t), bf) for t in range(stages)]
    scratch += [vmem(shape(t), bf) for t in range(stages)]
    scratch += [vmem(shape(t), f32) for t in range(stages)]
    scratch += [dma((3, 3)) for t in range(2 * stages)]
    outside = pl.BlockSpec(memory_space=pltpu.HBM)
    anywhere = pl.BlockSpec(memory_space=pl.ANY)
    result = pl.pallas_call(
        functools.partial(kernel, dims),
        out_shape=jax.ShapeDtypeStruct((high, 5 * edge), f32),
        in_specs=[outside] * 5,
        out_specs=anywhere,
        scratch_shapes=scratch,
        compiler_params=pltpu.CompilerParams(
            collective_id=0, has_side_effects=True, vmem_limit_bytes=44 * 1024 * 1024),
    )(*(pltpu.with_memory_space_constraint(x, pltpu.HBM) for x in (
        a_cols.transpose(2, 0, 1), p_cols.transpose(0, 2, 1), coarse_slot.T,
        a_blocks.reshape(rows * links, block, block), p_blocks.reshape(rows * kp, block, block))))
    return result.reshape(1, owned, block, 5 * edge)


def solution(mesh):
    return jax.shard_map(
        on_device,
        mesh=mesh,
        in_specs=(
            P("plane", "slab", None, None, None),
            P("plane", "slab", None),
            P("plane", "slab", None, None, None),
            P(),
            P(),
        ),
        out_specs=P("plane", "slab", None, None),
        check_vma=False,
    )
```
